16 devices in a mesh: dp: 1, sp: 16 (over x, y, z, core).
Axes of the slice: x: 2, y: 2, z: 2, core: 2. Of those that a mesh axis runs over, the one named last changes fastest.
Arguments:
- q: bfloat16 [32, 56, 128], P('dp')
- k: bfloat16 [32, 4096, 56, 128], P('dp', 'sp')
- v: bfloat16 [32, 4096, 56, 128], P('dp', 'sp')
Outputs:
- q: bfloat16 [32, 56, 128], P('dp')
All inputs are finite; a program needn't handle non-finite values.
Results may differ from the reference program's by a relative error of at most 0.012.
Values are sent between devices in bfloat16 or wider.
A program may use at most 2 GiB of HBM per device.

```python
import jax
import jax.numpy as jnp

BATCH = 32
CACHE = 4096
HEADS = 56
KV_HEADS = 56
HEAD = 128


def setup_inputs(seed: int = 0, part: int = 0) -> dict:
    kq, kk, kv = (jax.random.fold_in(k, part) for k in jax.random.split(jax.random.key(seed), 3))
    return {
        "q": (3 * jax.random.normal(kq, (BATCH, HEADS, HEAD), jnp.float32)).astype(jnp.bfloat16),
        "k": jax.random.normal(kk, (BATCH, CACHE, KV_HEADS, HEAD), jnp.float32).astype(jnp.bfloat16),
        "v": jax.random.normal(kv, (BATCH, CACHE, KV_HEADS, HEAD), jnp.float32).astype(jnp.bfloat16),
    }


def einsum(form, a, b):
    return jnp.einsum(form, a.astype(jnp.float32), b.astype(jnp.float32))


def reference(q, k, v):
    grouped = q.reshape(BATCH, KV_HEADS, -1, HEAD)
    scores = einsum("bgsd,bugd->bgsu", grouped, k) * HEAD**-0.5
    weights = jax.nn.softmax(scores, -1).astype(jnp.bfloat16)
    return einsum("bgsu,bugd->bgsd", weights, v).astype(jnp.bfloat16).reshape(BATCH, HEADS, HEAD)
```

```python
import functools

import jax
import jax.numpy as jnp
from jax import lax
from jax.experimental import pallas as pl
from jax.experimental.pallas import tpu as pltpu
from jax.sharding import PartitionSpec as P

F32, BF16 = jnp.float32, jnp.bfloat16
LOG2E = 1.4426950408889634
CHUNK = 32
SLOTS = 4
LAST = 2
DELAY = 4
LANES = 128


def kernel(n, scale, q_hbm, k_hbm, v_hbm, out, q, keys, values, mask, scores, high, part, stats, parts, allstats, in_sem, sums_sem, sumr_sem, res_sems, res_semr, all_sems):
    count, heads, head = out.shape
    rows = keys.shape[1]
    chunk = CHUNK * heads
    owned = pl.cdiv(count, n)
    early = count - LAST
    me = lax.axis_index("sp")

    def fetch(i, which):
        slot = lax.rem(i, SLOTS)
        cache, here = ((k_hbm, keys), (v_hbm, values))[which]
        return pltpu.make_async_copy(cache.at[pl.ds(i * rows, rows)], here.at[slot], in_sem.at[which, slot])

    q_copy = pltpu.make_async_copy(q_hbm, q, in_sem.at[2, 0])
    q_copy.start()
    fetch(0, 0).start()
    for i in range(1, SLOTS):
        fetch(i, 0).start()
        fetch(i - 1, 1).start()
    fetch(SLOTS - 1, 1).start()

    barrier = pltpu.get_barrier_semaphore()
    for step in range(1, n):
        pl.semaphore_signal(barrier, inc=1, device_id={"sp": lax.rem(me + step, n)})

    column = lax.broadcasted_iota(jnp.int32, (heads, chunk), 1).astype(F32)
    column = column - heads * jnp.floor((column + 0.5) * (1 / heads))
    row = lax.broadcasted_iota(jnp.int32, (heads, chunk), 0).astype(F32)
    mask[...] = jnp.where(column == row, jnp.inf, -jnp.inf)

    lane = lax.broadcasted_iota(jnp.int32, (heads, LANES), 1)
    line = lax.broadcasted_iota(jnp.int32, (heads, LANES), 0)
    own_lane = lane == line

    def score(i):
        slot = lax.rem(i, SLOTS)
        best = []

        def one(j):
            got = lax.dot_general(q[i], keys[slot, pl.ds(j * chunk, chunk), :], (((1,), (1,)), ((), ())), preferred_element_type=F32)
            got = jnp.minimum(got, mask[...])
            scores[:, pl.ds(j * chunk, chunk)] = got
            for g in range(chunk // LANES):
                piece = got[:, g * LANES : (g + 1) * LANES]
                best[:] = [jnp.maximum(best[0], piece) if best else piece]

        def end():
            high[...] = jnp.broadcast_to(jnp.max(best[0], -1, keepdims=True), (heads, LANES))

        return one, end

    def value(i):
        slot = lax.rem(i, SLOTS)
        top = high[...]
        total, seen = [], []

        def one(j):
            weights = []
            for g in range(chunk // LANES):
                w = jnp.exp2((scores[:, pl.ds(j * chunk + g * LANES, LANES)] - top) * (scale * LOG2E))
                total[:] = [total[0] + w if total else w]
                weights.append(w.astype(BF16))
            got = jnp.dot(jnp.concatenate(weights, 1), values[slot, pl.ds(j * chunk, chunk), :], preferred_element_type=F32)
            seen[:] = [seen[0] + got if seen else got]

        def end():
            sums = jnp.sum(total[0], -1, keepdims=True)
            part[i] = seen[0].astype(BF16)
            both = jnp.where(own_lane, top, 0.0) + jnp.where(lane == line + LANES // 2, sums, 0.0)
            stats[i] = jnp.sum(both, 0, keepdims=True)

        return one, end

    def part_copies(i, place, there, sems, semr):
        return [
            pltpu.make_async_remote_copy(part.at[i], parts.at[place, me], sems[0], semr[0], device_id={"sp": there}),
            pltpu.make_async_remote_copy(stats.at[i], allstats.at[place, me], sems[1], semr[1], device_id={"sp": there}),
        ]

    def to_owner(i):
        place = i // n
        return part_copies(
            i, place, lax.rem(i, n), (sums_sem.at[0, i], sums_sem.at[1, i]), (sumr_sem.at[0, place, me], sumr_sem.at[1, place, me])
        )

    def keep(i, place):
        parts[place, me] = part[i]
        allstats[place, me] = stats[i]

    def other(flips):
        there = me
        for bit in range(4):
            if flips >> bit & 1:
                there = there + (1 - 2 * lax.rem(me // 2**bit, 2)) * 2**bit
        return there

    order = sorted(range(1, n), key=lambda flips: (-bin(flips >> 1).count("1"), flips))

    def to_all(i, flips):
        which = i - early
        place = owned + which
        there = other(flips)
        return part_copies(
            i,
            place,
            there,
            (all_sems.at[0, which, flips], all_sems.at[1, which, flips]),
            (sumr_sem.at[0, place, me], sumr_sem.at[1, place, me]),
        )

    def arrived(place):
        for flips in order:
            there = other(flips)
            pltpu.make_async_copy(parts.at[place, there], parts.at[place, there], sumr_sem.at[0, place, there]).wait()
            pltpu.make_async_copy(allstats.at[place, there], allstats.at[place, there], sumr_sem.at[1, place, there]).wait()

    def combine(place, i):
        both = jnp.concatenate([allstats[place, s] for s in range(n)], 0)
        sums = pltpu.roll(both, LANES // 2, 1)
        share = jnp.exp2((both - jnp.max(both, 0, keepdims=True)) * (scale * LOG2E))
        share = share / jnp.sum(share * sums, 0, keepdims=True)
        got = None
        for s in range(n):
            mine = jnp.broadcast_to(share[s : s + 1], (heads, LANES))
            mine = jnp.sum(jnp.where(own_lane, mine, 0.0), -1, keepdims=True)
            term = mine * parts[place, s].astype(F32)
            got = term if got is None else got + term
        out[i] = got.astype(BF16)

    def result_copy(i, there, slot):
        return pltpu.make_async_remote_copy(
            out.at[i], out.at[i], res_sems.at[i // n, slot], res_semr.at[i], device_id={"sp": there}
        )

    def finish(i):
        @pl.when(lax.rem(i, n) == me)
        def _():
            place = i // n
            arrived(place)
            combine(place, i)
            for flips in order:
                result_copy(i, other(flips), flips).start()

    q_copy.wait()
    fetch(0, 0).wait()
    one, end = score(0)
    for j in range(rows // chunk):
        one(j)
    end()
    pl.semaphore_wait(barrier, n - 1)

    def step(i, _):
        @pl.when(jnp.logical_and(i >= 2, i + SLOTS - 2 < count))
        def _():
            fetch(i + SLOTS - 2, 1).start()

        @pl.when(i + SLOTS - 1 < count)
        def _():
            fetch(i + SLOTS - 1, 0).start()

        fetch(i, 0).wait()
        fetch(i - 1, 1).wait()
        value_one, value_end = value(i - 1)
        score_one, score_end = score(i)
        for j in range(rows // chunk):
            value_one(j)
            score_one(j)
        value_end()
        score_end()

        last = i - 1

        @pl.when(jnp.logical_and(last < early, lax.rem(last, n) != me))
        def _():
            for copy in to_owner(last):
                copy.start()

        @pl.when(jnp.logical_and(last < early, lax.rem(last, n) == me))
        def _():
            keep(last, last // n)

        for i_all in range(early, count - 1):

            @pl.when(last == i_all)
            def _():
                for flips in order:
                    for copy in to_all(i_all, flips):
                        copy.start()
                keep(i_all, owned + i_all - early)

        @pl.when(last >= DELAY)
        def _():
            finish(last - DELAY)

        return 0

    lax.fori_loop(1, count, step, 0)

    end_i = count - 1
    fetch(end_i, 1).wait()
    one, end = value(end_i)
    for j in range(rows // chunk):
        one(j)
    end()
    for flips in order:
        for copy in to_all(end_i, flips):
            copy.start()
    keep(end_i, owned + LAST - 1)

    for i in range(count - 1 - DELAY, early):
        finish(i)
    for i in range(early, count):
        arrived(owned + i - early)
        combine(owned + i - early, i)

    def ends(i, _):
        @pl.when(lax.rem(i, n) != me)
        def _():
            for copy in to_owner(i):
                copy.wait_send()
            result_copy(i, 0, 0).wait_recv()

        @pl.when(lax.rem(i, n) == me)
        def _():
            for flips in order:
                result_copy(i, other(flips), flips).wait_send()

        return 0

    lax.fori_loop(0, early, ends, 0)
    for i in range(early, count):
        for flips in order:
            for copy in to_all(i, flips):
                copy.wait_send()


def solution(mesh):
    n = mesh.shape["sp"]

    def step(q, k, v):
        count, tokens, heads, head = k.shape
        rows = tokens * heads
        owned = pl.cdiv(count, n)
        places = owned + LAST
        anywhere = pl.BlockSpec(memory_space=pl.ANY)
        dma = pltpu.SemaphoreType.DMA
        return pl.pallas_call(
            functools.partial(kernel, n, head**-0.5),
            out_shape=jax.ShapeDtypeStruct(q.shape, BF16),
            in_specs=[anywhere] * 3,
            out_specs=pl.BlockSpec(memory_space=pltpu.VMEM),
            scratch_shapes=[
                pltpu.VMEM(q.shape, BF16),
                pltpu.VMEM((SLOTS, rows, head), BF16),
                pltpu.VMEM((SLOTS, rows, head), BF16),
                pltpu.VMEM((heads, CHUNK * heads), F32),
                pltpu.VMEM((heads, rows), F32),
                pltpu.VMEM((heads, LANES), F32),
                pltpu.VMEM((count, heads, head), BF16),
                pltpu.VMEM((count, 1, LANES), F32),
                pltpu.VMEM((places, n, heads, head), BF16),
                pltpu.VMEM((places, n, 1, LANES), F32),
                dma((3, SLOTS)),
                dma((2, count)),
                dma((2, places, n)),
                dma((owned, n)),
                dma((count,)),
                dma((2, LAST, n)),
            ],
            compiler_params=pltpu.CompilerParams(collective_id=0, has_side_effects=True, vmem_limit_bytes=63 * 2**20),
        )(q, k.reshape(-1, head), v.reshape(-1, head))

    return jax.shard_map(
        step,
        mesh=mesh,
        in_specs=(P("dp", None, None), P("dp", "sp", None, None), P("dp", "sp", None, None)),
        out_specs=P("dp", None, None),
        check_vma=False,
    )
```

```python
import functools

import jax
import jax.numpy as jnp
from jax import lax
from jax.experimental import pallas as pl
from jax.experimental.pallas import tpu as pltpu
from jax.sharding import PartitionSpec as P

F32, BF16 = jnp.float32, jnp.bfloat16
LOG2E = 1.4426950408889634
CHUNK = 32
SLOTS = 4
LAST = 1
PIECES = 4
DELAY = 3
SENT = 6
LANES = 128


def kernel(n, scale, q_hbm, k_hbm, v_hbm, out, q, keys, values, mask, scores, high, part, stats, parts, allstats, in_sem, end_sem, to_sems, to_semr, res_sems, res_semr, all_sems):
    count, heads, head = out.shape
    rows = keys.shape[1]
    chunk = CHUNK * heads
    chunks = rows // chunk
    owned = pl.cdiv(count, n)
    early = count - LAST
    me = lax.axis_index("sp")

    def fetch(i, which):
        slot = lax.rem(i, SLOTS)
        cache, here = ((k_hbm, keys), (v_hbm, values))[which]
        return pltpu.make_async_copy(cache.at[pl.ds(i * rows, rows)], here.at[slot], in_sem.at[which, slot])

    def fetch_end(piece):
        size = rows // PIECES
        i = count - 1
        return pltpu.make_async_copy(
            v_hbm.at[pl.ds(i * rows + piece * size, size)],
            values.at[i % SLOTS, pl.ds(piece * size, size)],
            end_sem.at[piece],
        )

    q_copy = pltpu.make_async_copy(q_hbm, q, in_sem.at[2, 0])
    q_copy.start()
    fetch(0, 0).start()
    for i in range(1, SLOTS):
        fetch(i, 0).start()
        fetch(i - 1, 1).start()

    barrier = pltpu.get_barrier_semaphore()
    for step in range(1, n):
        pl.semaphore_signal(barrier, inc=1, device_id={"sp": lax.rem(me + step, n)})

    column = lax.broadcasted_iota(jnp.int32, (heads, chunk), 1).astype(F32)
    column = column - heads * jnp.floor((column + 0.5) * (1 / heads))
    row = lax.broadcasted_iota(jnp.int32, (heads, chunk), 0).astype(F32)
    mask[...] = jnp.where(column == row, jnp.inf, -jnp.inf)

    lane = lax.broadcasted_iota(jnp.int32, (heads, LANES), 1)
    line = lax.broadcasted_iota(jnp.int32, (heads, LANES), 0)
    own_lane = lane == line

    def score(i, place):
        slot = lax.rem(i, SLOTS)
        best = []

        def one(j):
            got = lax.dot_general(q[i], keys[slot, pl.ds(j * chunk, chunk), :], (((1,), (1,)), ((), ())), preferred_element_type=F32)
            got = jnp.minimum(got, mask[...])
            scores[place, :, pl.ds(j * chunk, chunk)] = got
            for g in range(chunk // LANES):
                piece = got[:, g * LANES : (g + 1) * LANES]
                best[:] = [jnp.maximum(best[0], piece) if best else piece]

        def end():
            high[place] = jnp.broadcast_to(jnp.max(best[0], -1, keepdims=True), (heads, LANES))

        return one, end

    def value(i, place):
        slot = lax.rem(i, SLOTS)
        top = high[place]
        total, seen = [], []

        def one(j):
            weights = []
            for g in range(chunk // LANES):
                w = jnp.exp2((scores[place, :, pl.ds(j * chunk + g * LANES, LANES)] - top) * (scale * LOG2E))
                total[:] = [total[0] + w if total else w]
                weights.append(w.astype(BF16))
            got = jnp.dot(jnp.concatenate(weights, 1), values[slot, pl.ds(j * chunk, chunk), :], preferred_element_type=F32)
            seen[:] = [seen[0] + got if seen else got]

        def end():
            sums = jnp.sum(total[0], -1, keepdims=True)
            part[i] = seen[0].astype(BF16)
            both = jnp.where(own_lane, top, 0.0) + jnp.where(lane == line + LANES // 2, sums, 0.0)
            stats[i] = jnp.sum(both, 0, keepdims=True)

        return one, end

    def part_copies(i, place, there, sems):
        return [
            pltpu.make_async_remote_copy(part.at[i], parts.at[place, me], sems[0], to_semr.at[0, place], device_id={"sp": there}),
            pltpu.make_async_remote_copy(stats.at[i], allstats.at[place, me], sems[1], to_semr.at[1, place], device_id={"sp": there}),
        ]

    def to_owner(i):
        return part_copies(i, i // n, lax.rem(i, n), (to_sems.at[0, i], to_sems.at[1, i]))

    def keep(i, place):
        parts[place, me] = part[i]
        allstats[place, me] = stats[i]

    def other(flips):
        there = me
        for bit in range(4):
            if flips >> bit & 1:
                there = there + (1 - 2 * lax.rem(me // 2**bit, 2)) * 2**bit
        return there

    order = sorted(range(1, n), key=lambda flips: (-bin(flips >> 1).count("1"), flips))

    def to_all(i):
        which = i - early
        for flips in order:
            for copy in part_copies(i, owned + which, other(flips), (all_sems.at[0, which], all_sems.at[1, which])):
                copy.start()
        keep(i, owned + which)

    def all_bytes(sem_part, sem_stats):
        for ref, sem in ((parts, sem_part), (allstats, sem_stats)):
            ref = ref.at[0, pl.ds(0, n - 1)]
            pltpu.make_async_copy(ref, ref, sem).wait()

    def combine(place, i):
        all_bytes(to_semr.at[0, place], to_semr.at[1, place])
        both = jnp.concatenate([allstats[place, s] for s in range(n)], 0)
        sums = pltpu.roll(both, LANES // 2, 1)
        share = jnp.exp2((both - jnp.max(both, 0, keepdims=True)) * (scale * LOG2E))
        share = share / jnp.sum(share * sums, 0, keepdims=True)
        got = None
        for s in range(n):
            mine = jnp.broadcast_to(share[s : s + 1], (heads, LANES))
            mine = jnp.sum(jnp.where(own_lane, mine, 0.0), -1, keepdims=True)
            term = mine * parts[place, s].astype(F32)
            got = term if got is None else got + term
        out[i] = got.astype(BF16)

    def finish(i):
        @pl.when(lax.rem(i, n) == me)
        def _():
            place = i // n
            combine(place, i)
            for flips in order:
                pltpu.make_async_remote_copy(out.at[i], out.at[i], res_sems.at[place], res_semr.at[0], device_id={"sp": other(flips)}).start()

    def sent(i):
        @pl.when(lax.rem(i, n) != me)
        def _():
            for copy in to_owner(i):
                copy.wait_send()

    q_copy.wait()
    fetch(0, 0).wait()
    one, end = score(0, 0)
    for j in range(chunks):
        one(j)
    end()
    pl.semaphore_wait(barrier, n - 1)

    def step(i, _):
        @pl.when(i < count - 5)
        def _():
            fetch(i + SLOTS - 2, 1).start()
            fetch(i + SLOTS - 1, 0).start()

        @pl.when(i == count - 5)
        def _():
            fetch(count - 2, 0).start()

        @pl.when(i == count - 4)
        def _():
            fetch(count - 1, 0).start()
            fetch(count - 3, 1).start()
            fetch(count - 2, 1).start()

        @pl.when(i == count - 3)
        def _():
            for piece in range(PIECES):
                fetch_end(piece).start()

        fetch(i, 0).wait()
        fetch(i - 1, 1).wait()
        value_one, value_end = value(i - 1, 0)
        score_one, score_end = score(i, 0)
        for j in range(chunks):
            value_one(j)
            score_one(j)
        value_end()
        score_end()

        last = i - 1

        @pl.when(lax.rem(last, n) != me)
        def _():
            for copy in to_owner(last):
                copy.start()

        @pl.when(lax.rem(last, n) == me)
        def _():
            keep(last, last // n)

        @pl.when(last >= DELAY)
        def _():
            finish(last - DELAY)

        @pl.when(last >= SENT)
        def _():
            sent(last - SENT)

        return 0

    lax.fori_loop(1, count - 2, step, 0)

    for place, i in enumerate((count - 2, count - 1), 1):
        fetch(i, 0).wait()
        one, end = score(i, place)
        for j in range(chunks):
            one(j)
        end()
        if count - 3 - DELAY + place - 1 < early - 1:
            finish(count - 3 - DELAY + place - 1)

    for place, i in enumerate((count - 3, count - 2, count - 1)):
        pieces = PIECES if i == count - 1 else 1
        one, end = value(i, place)
        for piece in range(pieces):
            if i == count - 1:
                fetch_end(piece).wait()
            else:
                fetch(i, 1).wait()
            for j in range(piece * chunks // pieces, (piece + 1) * chunks // pieces):
                one(j)
        end()
        if i < early:
            @pl.when(lax.rem(i, n) != me)
            def _():
                for copy in to_owner(i):
                    copy.start()

            @pl.when(lax.rem(i, n) == me)
            def _():
                keep(i, i // n)
        else:
            to_all(i)

    for i in range(count - 3 - DELAY + 2, early):
        finish(i)
    for i in range(early, count):
        combine(owned + i - early, i)

    for i in range(count - 3 - SENT, early):
        sent(i)
    most = pl.cdiv(early, n)
    for mine in (most - 1, most):
        @pl.when((early + n - 1 - me) // n == mine)
        def _():
            ref = out.at[pl.ds(0, early - mine)]
            pltpu.make_async_copy(ref, ref, res_semr.at[0]).wait()
            ref = out.at[pl.ds(0, n - 1)]
            for place in range(mine):
                pltpu.make_async_copy(ref, ref, res_sems.at[place]).wait()

    for which in range(LAST):
        all_bytes(all_sems.at[0, which], all_sems.at[1, which])


def solution(mesh):
    n = mesh.shape["sp"]

    def step(q, k, v):
        count, tokens, heads, head = k.shape
        rows = tokens * heads
        owned = pl.cdiv(count, n)
        places = owned + LAST
        anywhere = pl.BlockSpec(memory_space=pl.ANY)
        dma = pltpu.SemaphoreType.DMA
        return pl.pallas_call(
            functools.partial(kernel, n, head**-0.5),
            out_shape=jax.ShapeDtypeStruct(q.shape, BF16),
            in_specs=[pl.BlockSpec(memory_space=pltpu.HBM), anywhere, anywhere],
            out_specs=pl.BlockSpec(memory_space=pltpu.VMEM),
            scratch_shapes=[
                pltpu.VMEM(q.shape, BF16),
                pltpu.VMEM((SLOTS, rows, head), BF16),
                pltpu.VMEM((SLOTS, rows, head), BF16),
                pltpu.VMEM((heads, CHUNK * heads), F32),
                pltpu.VMEM((3, heads, rows), F32),
                pltpu.VMEM((3, heads, LANES), F32),
                pltpu.VMEM((count, heads, head), BF16),
                pltpu.VMEM((count, 1, LANES), F32),
                pltpu.VMEM((places, n, heads, head), BF16),
                pltpu.VMEM((places, n, 1, LANES), F32),
                dma((3, SLOTS)),
                dma((PIECES,)),
                dma((2, count)),
                dma((2, places)),
                dma((owned,)),
                dma((1,)),
                dma((2, LAST)),
            ],
            compiler_params=pltpu.CompilerParams(collective_id=0, has_side_effects=True, vmem_limit_bytes=48 * 2**20),
        )(pltpu.with_memory_space_constraint(q, pltpu.HBM), k.reshape(-1, head), v.reshape(-1, head))

    return jax.shard_map(
        step,
        mesh=mesh,
        in_specs=(P("dp", None, None), P("dp", "sp", None, None), P("dp", "sp", None, None)),
        out_specs=P("dp", None, None),
        check_vma=False,
    )
```

```python
import functools

import jax
import jax.numpy as jnp
from jax import lax
from jax.experimental import pallas as pl
from jax.experimental.pallas import tpu as pltpu
from jax.sharding import PartitionSpec as P

F32, BF16 = jnp.float32, jnp.bfloat16
LOG2E = 1.4426950408889634
CHUNK = 32
SLOTS = 4
LAST = 3
PIECES = 4
DELAY = 3
SENT = 6
LANES = 128


def kernel(n, scale, q_hbm, k_hbm, v_hbm, out, q, keys, values, mask, scores, high, part, stats, parts, allstats, in_sem, end_sem, to_sems, to_semr, res_sems, res_semr, mine, halves, pair, pairstats, both, bothstats, alls, allsstats, pair_sems, pair_semr, all_sems, all_semr):
    count, heads, head = out.shape
    rows = keys.shape[1]
    chunk = CHUNK * heads
    chunks = rows // chunk
    owned = pl.cdiv(count, n)
    early = count - LAST
    me = lax.axis_index("sp")

    def fetch(i, which):
        slot = lax.rem(i, SLOTS)
        cache, here = ((k_hbm, keys), (v_hbm, values))[which]
        return pltpu.make_async_copy(cache.at[pl.ds(i * rows, rows)], here.at[slot], in_sem.at[which, slot])

    def fetch_end(piece):
        size = rows // PIECES
        i = count - 1
        return pltpu.make_async_copy(
            v_hbm.at[pl.ds(i * rows + piece * size, size)],
            values.at[i % SLOTS, pl.ds(piece * size, size)],
            end_sem.at[piece],
        )

    q_copy = pltpu.make_async_copy(q_hbm, q, in_sem.at[2, 0])
    q_copy.start()
    fetch(0, 0).start()
    for i in range(1, SLOTS):
        fetch(i, 0).start()
        fetch(i - 1, 1).start()

    barrier = pltpu.get_barrier_semaphore()
    for step in range(1, n):
        pl.semaphore_signal(barrier, inc=1, device_id={"sp": lax.rem(me + step, n)})

    column = lax.broadcasted_iota(jnp.int32, (heads, chunk), 1).astype(F32)
    column = column - heads * jnp.floor((column + 0.5) * (1 / heads))
    row = lax.broadcasted_iota(jnp.int32, (heads, chunk), 0).astype(F32)
    mask[...] = jnp.where(column == row, jnp.inf, -jnp.inf)

    lane = lax.broadcasted_iota(jnp.int32, (heads, LANES), 1)
    line = lax.broadcasted_iota(jnp.int32, (heads, LANES), 0)
    own_lane = lane == line

    def score(i, place):
        slot = lax.rem(i, SLOTS)
        best = []

        def one(j):
            got = lax.dot_general(q[i], keys[slot, pl.ds(j * chunk, chunk), :], (((1,), (1,)), ((), ())), preferred_element_type=F32)
            got = jnp.minimum(got, mask[...])
            scores[place, :, pl.ds(j * chunk, chunk)] = got
            for g in range(chunk // LANES):
                piece = got[:, g * LANES : (g + 1) * LANES]
                best[:] = [jnp.maximum(best[0], piece) if best else piece]

        def end():
            high[place] = jnp.broadcast_to(jnp.max(best[0], -1, keepdims=True), (heads, LANES))

        return one, end

    def value(i, place):
        slot = lax.rem(i, SLOTS)
        top = high[place]
        total, seen = [], []

        def one(j):
            weights = []
            for g in range(chunk // LANES):
                w = jnp.exp2((scores[place, :, pl.ds(j * chunk + g * LANES, LANES)] - top) * (scale * LOG2E))
                total[:] = [total[0] + w if total else w]
                weights.append(w.astype(BF16))
            got = jnp.dot(jnp.concatenate(weights, 1), values[slot, pl.ds(j * chunk, chunk), :], preferred_element_type=F32)
            seen[:] = [seen[0] + got if seen else got]

        def end():
            sums = jnp.sum(total[0], -1, keepdims=True)
            known = jnp.where(own_lane, top, 0.0) + jnp.where(lane == line + LANES // 2, sums, 0.0)
            stats[i] = jnp.sum(known, 0, keepdims=True)
            return seen[0]

        return one, end

    def part_copies(i, place, there, sems):
        return [
            pltpu.make_async_remote_copy(part.at[i], parts.at[place, me], sems[0], to_semr.at[0, place], device_id={"sp": there}),
            pltpu.make_async_remote_copy(stats.at[i], allstats.at[place, me], sems[1], to_semr.at[1, place], device_id={"sp": there}),
        ]

    def to_owner(i):
        return part_copies(i, i // n, lax.rem(i, n), (to_sems.at[0, i], to_sems.at[1, i]))

    def keep(i, place):
        parts[place, me] = part[i]
        allstats[place, me] = stats[i]

    def other(flips):
        there = me
        for bit in range(4):
            if flips >> bit & 1:
                there = there + (1 - 2 * lax.rem(me // 2**bit, 2)) * 2**bit
        return there

    order = sorted(range(1, n), key=lambda flips: (-bin(flips >> 1).count("1"), flips))

    core = lax.rem(me, 2)
    half = halves.shape[2]
    cuts = (0, heads - half)
    line_half = lax.broadcasted_iota(jnp.int32, (half, LANES), 0)
    lane_half = lax.broadcasted_iota(jnp.int32, (half, LANES), 1)
    low = lax.broadcasted_iota(jnp.int32, (1, LANES), 1) < LANES // 2

    def swap(which, i):
        there = other(1)
        return [
            pltpu.make_async_remote_copy(halves.at[which, 1 - core], pair.at[which], pair_sems.at[0, which], pair_semr.at[0, which], device_id={"sp": there}),
            pltpu.make_async_remote_copy(stats.at[i], pairstats.at[which], pair_sems.at[1, which], pair_semr.at[1, which], device_id={"sp": there}),
        ]

    def to_pair(i, seen):
        which = i - early
        for c, cut in enumerate(cuts):
            mine[which, c] = seen[cut : cut + half]
            halves[which, c] = seen[cut : cut + half].astype(BF16)
        for copy in swap(which, i):
            copy.start()

    def all_copies(which, there):
        return [
            pltpu.make_async_remote_copy(both.at[which], alls.at[which, me], all_sems.at[0, which], all_semr.at[0, which], device_id={"sp": there}),
            pltpu.make_async_remote_copy(bothstats.at[which], allsstats.at[which, me], all_sems.at[1, which], all_semr.at[1, which], device_id={"sp": there}),
        ]

    def to_all(i):
        which = i - early
        for copy in swap(which, i):
            copy.wait_recv()
        a, b = stats[i], pairstats[which]
        top = jnp.maximum(a, b)
        a_share, b_share = jnp.exp2((a - top) * (scale * LOG2E)), jnp.exp2((b - top) * (scale * LOG2E))
        sums = a_share * pltpu.roll(a, LANES // 2, 1) + b_share * pltpu.roll(b, LANES // 2, 1)
        known = jnp.where(low, top, pltpu.roll(sums, LANES // 2, 1))
        own = lane_half == line_half + core * cuts[1]
        a_share, b_share = (jnp.sum(jnp.where(own, jnp.broadcast_to(x, own.shape), 0.0), -1, keepdims=True) for x in (a_share, b_share))
        got = (a_share * mine[which, core] + b_share * pair[which].astype(F32)).astype(BF16)
        both[which] = got
        bothstats[which] = known
        for flips in order:
            for copy in all_copies(which, other(flips)):
                copy.start()
        alls[which, me] = got
        allsstats[which, me] = known

    def combine_all(i):
        which = i - early
        some_bytes(alls, all_semr.at[0, which])
        some_bytes(allsstats, all_semr.at[1, which])
        done = []
        for c, cut in enumerate(cuts):
            share = shares(jnp.concatenate([allsstats[which, s] for s in range(c, n, 2)], 0))
            start = half - cut if c else 0
            own = own_lane[cut + start : cut + half]
            got = None
            for j, s in enumerate(range(c, n, 2)):
                column = jnp.sum(jnp.where(own, jnp.broadcast_to(share[j : j + 1], own.shape), 0.0), -1, keepdims=True)
                term = column * alls[which, s].astype(F32)[start:]
                got = term if got is None else got + term
            done.append(got)
        out[i] = jnp.concatenate(done, 0).astype(BF16)

    def some_bytes(ref, sem):
        ref = ref.at[0, pl.ds(0, n - 1)]
        pltpu.make_async_copy(ref, ref, sem).wait()

    def shares(known):
        share = jnp.exp2((known - jnp.max(known, 0, keepdims=True)) * (scale * LOG2E))
        return share / jnp.sum(share * pltpu.roll(known, LANES // 2, 1), 0, keepdims=True)

    def combine(place, i):
        some_bytes(parts, to_semr.at[0, place])
        some_bytes(allstats, to_semr.at[1, place])
        share = shares(jnp.concatenate([allstats[place, s] for s in range(n)], 0))
        got = None
        for s in range(n):
            column = jnp.sum(jnp.where(own_lane, jnp.broadcast_to(share[s : s + 1], (heads, LANES)), 0.0), -1, keepdims=True)
            term = column * parts[place, s].astype(F32)
            got = term if got is None else got + term
        out[i] = got.astype(BF16)

    def finish(i):
        @pl.when(lax.rem(i, n) == me)
        def _():
            place = i // n
            combine(place, i)
            for flips in order:
                pltpu.make_async_remote_copy(out.at[i], out.at[i], res_sems.at[place], res_semr.at[0], device_id={"sp": other(flips)}).start()

    def sent(i):
        @pl.when(lax.rem(i, n) != me)
        def _():
            for copy in to_owner(i):
                copy.wait_send()

    q_copy.wait()
    fetch(0, 0).wait()
    one, end = score(0, 0)
    for j in range(chunks):
        one(j)
    end()
    pl.semaphore_wait(barrier, n - 1)

    def step(i, _):
        @pl.when(i < count - 5)
        def _():
            fetch(i + SLOTS - 2, 1).start()
            fetch(i + SLOTS - 1, 0).start()

        @pl.when(i == count - 5)
        def _():
            fetch(count - 2, 0).start()

        @pl.when(i == count - 4)
        def _():
            fetch(count - 1, 0).start()
            fetch(count - 3, 1).start()
            fetch(count - 2, 1).start()

        @pl.when(i == count - 3)
        def _():
            for piece in range(PIECES):
                fetch_end(piece).start()

        fetch(i, 0).wait()
        fetch(i - 1, 1).wait()
        value_one, value_end = value(i - 1, 0)
        score_one, score_end = score(i, 0)
        for j in range(chunks):
            value_one(j)
            score_one(j)
        last = i - 1
        part[last] = value_end().astype(BF16)
        score_end()

        @pl.when(lax.rem(last, n) != me)
        def _():
            for copy in to_owner(last):
                copy.start()

        @pl.when(lax.rem(last, n) == me)
        def _():
            keep(last, last // n)

        @pl.when(last >= DELAY)
        def _():
            finish(last - DELAY)

        @pl.when(last >= SENT)
        def _():
            sent(last - SENT)

        return 0

    lax.fori_loop(1, count - 2, step, 0)

    for place, i in enumerate((count - 2, count - 1), 1):
        fetch(i, 0).wait()
        one, end = score(i, place)
        for j in range(chunks):
            one(j)
        end()
        if count - 3 - DELAY + place - 1 < early - 1:
            finish(count - 3 - DELAY + place - 1)

    for place, i in enumerate((count - 3, count - 2, count - 1)):
        pieces = PIECES if i == count - 1 else 1
        one, end = value(i, place)
        for piece in range(pieces):
            if i == count - 1:
                fetch_end(piece).wait()
            else:
                fetch(i, 1).wait()
            for j in range(piece * chunks // pieces, (piece + 1) * chunks // pieces):
                one(j)
        to_pair(i, end())
        if i > early:
            to_all(i - 1)
    for i in range(count - 3 - DELAY + 2, early):
        finish(i)
    to_all(count - 1)
    for i in range(early, count):
        combine_all(i)

    for i in range(count - 3 - SENT, early):
        sent(i)
    most = pl.cdiv(early, n)
    for number in (most - 1, most):

        @pl.when((early + n - 1 - me) // n == number)
        def _():
            ref = out.at[pl.ds(0, early - number)]
            pltpu.make_async_copy(ref, ref, res_semr.at[0]).wait()
            ref = out.at[pl.ds(0, n - 1)]
            for place in range(number):
                pltpu.make_async_copy(ref, ref, res_sems.at[place]).wait()

    for which in range(LAST):
        for copy in swap(which, early + which):
            copy.wait_send()
        some_bytes(alls, all_sems.at[0, which])
        some_bytes(allsstats, all_sems.at[1, which])


def solution(mesh):
    n = mesh.shape["sp"]

    def step(q, k, v):
        count, tokens, heads, head = k.shape
        rows = tokens * heads
        owned = pl.cdiv(count, n)
        half = heads * 4 // 7
        anywhere = pl.BlockSpec(memory_space=pl.ANY)
        dma = pltpu.SemaphoreType.DMA
        return pl.pallas_call(
            functools.partial(kernel, n, head**-0.5),
            out_shape=jax.ShapeDtypeStruct(q.shape, BF16),
            in_specs=[pl.BlockSpec(memory_space=pltpu.HBM), anywhere, anywhere],
            out_specs=pl.BlockSpec(memory_space=pltpu.VMEM),
            scratch_shapes=[
                pltpu.VMEM(q.shape, BF16),
                pltpu.VMEM((SLOTS, rows, head), BF16),
                pltpu.VMEM((SLOTS, rows, head), BF16),
                pltpu.VMEM((heads, CHUNK * heads), F32),
                pltpu.VMEM((3, heads, rows), F32),
                pltpu.VMEM((3, heads, LANES), F32),
                pltpu.VMEM((count, heads, head), BF16),
                pltpu.VMEM((count, 1, LANES), F32),
                pltpu.VMEM((owned, n, heads, head), BF16),
                pltpu.VMEM((owned, n, 1, LANES), F32),
                dma((3, SLOTS)),
                dma((PIECES,)),
                dma((2, count)),
                dma((2, owned)),
                dma((owned,)),
                dma((1,)),
                pltpu.VMEM((LAST, 2, half, head), F32),
                pltpu.VMEM((LAST, 2, half, head), BF16),
                pltpu.VMEM((LAST, half, head), BF16),
                pltpu.VMEM((LAST, 1, LANES), F32),
                pltpu.VMEM((LAST, half, head), BF16),
                pltpu.VMEM((LAST, 1, LANES), F32),
                pltpu.VMEM((LAST, n, half, head), BF16),
                pltpu.VMEM((LAST, n, 1, LANES), F32),
                dma((2, LAST)),
                dma((2, LAST)),
                dma((2, LAST)),
                dma((2, LAST)),
            ],
            compiler_params=pltpu.CompilerParams(collective_id=0, has_side_effects=True, vmem_limit_bytes=48 * 2**20),
        )(pltpu.with_memory_space_constraint(q, pltpu.HBM), k.reshape(-1, head), v.reshape(-1, head))

    return jax.shard_map(
        step,
        mesh=mesh,
        in_specs=(P("dp", None, None), P("dp", "sp", None, None), P("dp", "sp", None, None)),
        out_specs=P("dp", None, None),
        check_vma=False,
    )
```

```python
import functools

import jax
import jax.numpy as jnp
from jax import lax
from jax.experimental import pallas as pl
from jax.experimental.pallas import tpu as pltpu
from jax.sharding import PartitionSpec as P

F32, BF16 = jnp.float32, jnp.bfloat16
LOG2E = 1.4426950408889634
CHUNK = 32
SLOTS = 4
LAST = 3
DELAY = 3
SENT = 3
LANES = 128


def kernel(n, scale, q_hbm, k_hbm, v_hbm, out, q, keys, values, mask, scores, high, part, stats, parts, allstats, in_sem, to_sems, to_semr, res_sems, res_semr, mine, halves, pair, pairstats, both, bothstats, alls, allsstats, pair_sems, pair_semr, all_sems, all_semr):
    count, heads, head = out.shape
    rows = keys.shape[1]
    chunk = CHUNK * heads
    chunks = rows // chunk
    owned = pl.cdiv(count, n)
    early = count - LAST
    me = lax.axis_index("sp")

    def fetch(i, which):
        slot = lax.rem(i, SLOTS)
        cache, here = ((k_hbm, keys), (v_hbm, values))[which]
        return pltpu.make_async_copy(cache.at[pl.ds(i * rows, rows)], here.at[slot], in_sem.at[which, slot])

    q_copy = pltpu.make_async_copy(q_hbm, q, in_sem.at[2, 0])
    q_copy.start()
    fetch(0, 0).start()
    for i in range(1, SLOTS):
        fetch(i, 0).start()
        fetch(i - 1, 1).start()

    barrier = pltpu.get_barrier_semaphore()
    for step in range(1, n):
        pl.semaphore_signal(barrier, inc=1, device_id={"sp": lax.rem(me + step, n)})

    column = lax.broadcasted_iota(jnp.int32, (heads, chunk), 1).astype(F32)
    column = column - heads * jnp.floor((column + 0.5) * (1 / heads))
    row = lax.broadcasted_iota(jnp.int32, (heads, chunk), 0).astype(F32)
    mask[...] = jnp.where(column == row, jnp.inf, -jnp.inf)

    lane = lax.broadcasted_iota(jnp.int32, (heads, LANES), 1)
    line = lax.broadcasted_iota(jnp.int32, (heads, LANES), 0)
    own_lane = lane == line

    def score(i, place):
        slot = lax.rem(i, SLOTS)
        best = []

        def one(j):
            got = lax.dot_general(q[i], keys[slot, pl.ds(j * chunk, chunk), :], (((1,), (1,)), ((), ())), preferred_element_type=F32)
            got = jnp.minimum(got, mask[...])
            scores[place, :, pl.ds(j * chunk, chunk)] = got
            for g in range(chunk // LANES):
                piece = got[:, g * LANES : (g + 1) * LANES]
                best[:] = [jnp.maximum(best[0], piece) if best else piece]

        def end():
            high[place] = jnp.broadcast_to(jnp.max(best[0], -1, keepdims=True), (heads, LANES))

        return one, end

    def value(i, place):
        slot = lax.rem(i, SLOTS)
        top = high[place]
        total, seen = [], []

        def one(j):
            weights = []
            for g in range(chunk // LANES):
                w = jnp.exp2((scores[place, :, pl.ds(j * chunk + g * LANES, LANES)] - top) * (scale * LOG2E))
                total[:] = [total[0] + w if total else w]
                weights.append(w.astype(BF16))
            got = jnp.dot(jnp.concatenate(weights, 1), values[slot, pl.ds(j * chunk, chunk), :], preferred_element_type=F32)
            seen[:] = [seen[0] + got if seen else got]

        def end():
            sums = jnp.sum(total[0], -1, keepdims=True)
            known = jnp.where(own_lane, top, 0.0) + jnp.where(lane == line + LANES // 2, sums, 0.0)
            stats[i] = jnp.sum(known, 0, keepdims=True)
            return seen[0]

        return one, end

    def part_copies(i, place, there, sems):
        return [
            pltpu.make_async_remote_copy(part.at[i], parts.at[place, me], sems[0], to_semr.at[0, place], device_id={"sp": there}),
            pltpu.make_async_remote_copy(stats.at[i], allstats.at[place, me], sems[1], to_semr.at[1, place], device_id={"sp": there}),
        ]

    def owner(i):
        return lax.rem(i, n // 2) * 2 + lax.rem(i // (n // 2), 2)

    def to_owner(i):
        return part_copies(i, i // n, owner(i), (to_sems.at[0, lax.rem(i, SENT + 1)], to_sems.at[1, lax.rem(i, SENT + 1)]))

    def keep(i, place):
        parts[place, me] = part[i]
        allstats[place, me] = stats[i]

    def other(flips):
        there = me
        for bit in range(4):
            if flips >> bit & 1:
                there = there + (1 - 2 * lax.rem(me // 2**bit, 2)) * 2**bit
        return there

    order = sorted(range(1, n), key=lambda flips: (-bin(flips >> 1).count("1"), flips))

    core = lax.rem(me, 2)
    half = halves.shape[2]
    cuts = (0, heads - half)
    line_half = lax.broadcasted_iota(jnp.int32, (half, LANES), 0)
    lane_half = lax.broadcasted_iota(jnp.int32, (half, LANES), 1)
    low = lax.broadcasted_iota(jnp.int32, (1, LANES), 1) < LANES // 2

    def swap(which, i):
        there = other(1)
        return [
            pltpu.make_async_remote_copy(halves.at[which, 1 - core], pair.at[which], pair_sems.at[0, which], pair_semr.at[0, which], device_id={"sp": there}),
            pltpu.make_async_remote_copy(stats.at[i], pairstats.at[which], pair_sems.at[1, which], pair_semr.at[1, which], device_id={"sp": there}),
        ]

    def to_pair(i, seen):
        which = i - early
        for c, cut in enumerate(cuts):
            mine[which, c] = seen[cut : cut + half]
            halves[which, c] = seen[cut : cut + half].astype(BF16)
        for copy in swap(which, i):
            copy.start()

    def all_copies(which, there):
        return [
            pltpu.make_async_remote_copy(both.at[which], alls.at[which, me], all_sems.at[0, which], all_semr.at[0, which], device_id={"sp": there}),
            pltpu.make_async_remote_copy(bothstats.at[which], allsstats.at[which, me], all_sems.at[1, which], all_semr.at[1, which], device_id={"sp": there}),
        ]

    def to_all(i):
        which = i - early
        for copy in swap(which, i):
            copy.wait_recv()
        a, b = stats[i], pairstats[which]
        top = jnp.maximum(a, b)
        a_share, b_share = jnp.exp2((a - top) * (scale * LOG2E)), jnp.exp2((b - top) * (scale * LOG2E))
        sums = a_share * pltpu.roll(a, LANES // 2, 1) + b_share * pltpu.roll(b, LANES // 2, 1)
        known = jnp.where(low, top, pltpu.roll(sums, LANES // 2, 1))
        own = lane_half == line_half + core * cuts[1]
        a_share, b_share = (jnp.sum(jnp.where(own, jnp.broadcast_to(x, own.shape), 0.0), -1, keepdims=True) for x in (a_share, b_share))
        got = (a_share * mine[which, core] + b_share * pair[which].astype(F32)).astype(BF16)
        both[which] = got
        bothstats[which] = known
        for flips in order:
            for copy in all_copies(which, other(flips)):
                copy.start()
        alls[which, me] = got
        allsstats[which, me] = known

    def combine_all(i):
        which = i - early
        some_bytes(alls, all_semr.at[0, which])
        some_bytes(allsstats, all_semr.at[1, which])
        done = []
        for c, cut in enumerate(cuts):
            share = shares(jnp.concatenate([allsstats[which, s] for s in range(c, n, 2)], 0))
            start = half - cut if c else 0
            own = own_lane[cut + start : cut + half]
            got = None
            for j, s in enumerate(range(c, n, 2)):
                column = jnp.sum(jnp.where(own, jnp.broadcast_to(share[j : j + 1], own.shape), 0.0), -1, keepdims=True)
                term = column * alls[which, s].astype(F32)[start:]
                got = term if got is None else got + term
            done.append(got)
        out[i] = jnp.concatenate(done, 0).astype(BF16)

    def some_bytes(ref, sem):
        ref = ref.at[0, pl.ds(0, n - 1)]
        pltpu.make_async_copy(ref, ref, sem).wait()

    def shares(known):
        share = jnp.exp2((known - jnp.max(known, 0, keepdims=True)) * (scale * LOG2E))
        return share / jnp.sum(share * pltpu.roll(known, LANES // 2, 1), 0, keepdims=True)

    def combine(place, i):
        some_bytes(parts, to_semr.at[0, place])
        some_bytes(allstats, to_semr.at[1, place])
        share = shares(jnp.concatenate([allstats[place, s] for s in range(n)], 0))
        got = None
        for s in range(n):
            column = jnp.sum(jnp.where(own_lane, jnp.broadcast_to(share[s : s + 1], (heads, LANES)), 0.0), -1, keepdims=True)
            term = column * parts[place, s].astype(F32)
            got = term if got is None else got + term
        out[i] = got.astype(BF16)

    def finish(i):
        @pl.when(owner(i) == me)
        def _():
            place = i // n
            combine(place, i)
            for flips in order:
                pltpu.make_async_remote_copy(out.at[i], out.at[i], res_sems.at[place], res_semr.at[0], device_id={"sp": other(flips)}).start()

    def send(i):
        @pl.when(owner(i) != me)
        def _():
            for copy in to_owner(i):
                copy.start()

        @pl.when(owner(i) == me)
        def _():
            keep(i, i // n)

    def sent(i):
        @pl.when(owner(i) != me)
        def _():
            for copy in to_owner(i):
                copy.wait_send()

    q_copy.wait()
    fetch(0, 0).wait()
    one, end = score(0, 0)
    for j in range(chunks):
        one(j)
    end()
    pl.semaphore_wait(barrier, n - 1)

    def step(i, _):
        fetch(i + SLOTS - 2, 1).start()

        @pl.when(i + SLOTS - 1 < count)
        def _():
            fetch(i + SLOTS - 1, 0).start()

        fetch(i, 0).wait()
        fetch(i - 1, 1).wait()
        value_one, value_end = value(i - 1, 0)
        score_one, score_end = score(i, 0)
        for j in range(chunks):
            value_one(j)
            score_one(j)
        last = i - 1
        part[last] = value_end().astype(BF16)
        score_end()

        send(last)

        @pl.when(last >= DELAY)
        def _():
            finish(last - DELAY)

        @pl.when(last >= SENT)
        def _():
            sent(last - SENT)

        return 0

    lax.fori_loop(1, count - 2, step, 0)

    def score_alone(i, place):
        fetch(i, 0).wait()
        one, end = score(i, place)
        for j in range(chunks):
            one(j)
        end()

    def value_alone(i, place):
        fetch(i, 1).wait()
        one, end = value(i, place)
        for j in range(chunks):
            one(j)
        return end()

    a, b, c = range(early, count)
    score_alone(b, 1)
    finish(early - 3)
    to_pair(a, value_alone(a, 0))
    score_alone(c, 0)
    to_all(a)
    finish(early - 2)
    to_pair(b, value_alone(b, 1))
    finish(early - 1)
    to_pair(c, value_alone(c, 0))
    to_all(b)
    to_all(c)
    for i in range(early, count):
        combine_all(i)

    for i in range(early - SENT, early):
        sent(i)
    most = pl.cdiv(early, n)
    for number in (most - 1, most):

        @pl.when((early + n - 1 - me // 2 - lax.rem(me, 2) * (n // 2)) // n == number)
        def _():
            ref = out.at[pl.ds(0, early - number)]
            pltpu.make_async_copy(ref, ref, res_semr.at[0]).wait()
            ref = out.at[pl.ds(0, n - 1)]
            for place in range(number):
                pltpu.make_async_copy(ref, ref, res_sems.at[place]).wait()

    for which in range(LAST):
        for copy in swap(which, early + which):
            copy.wait_send()
        some_bytes(alls, all_sems.at[0, which])
        some_bytes(allsstats, all_sems.at[1, which])


def solution(mesh):
    n = mesh.shape["sp"]

    def step(q, k, v):
        count, tokens, heads, head = k.shape
        rows = tokens * heads
        owned = pl.cdiv(count, n)
        half = heads * 4 // 7
        anywhere = pl.BlockSpec(memory_space=pl.ANY)
        dma = pltpu.SemaphoreType.DMA
        return pl.pallas_call(
            functools.partial(kernel, n, head**-0.5),
            out_shape=jax.ShapeDtypeStruct(q.shape, BF16),
            in_specs=[pl.BlockSpec(memory_space=pltpu.HBM), anywhere, anywhere],
            out_specs=pl.BlockSpec(memory_space=pltpu.VMEM),
            scratch_shapes=[
                pltpu.VMEM(q.shape, BF16),
                pltpu.VMEM((SLOTS, rows, head), BF16),
                pltpu.VMEM((SLOTS, rows, head), BF16),
                pltpu.VMEM((heads, CHUNK * heads), F32),
                pltpu.VMEM((2, heads, rows), F32),
                pltpu.VMEM((2, heads, LANES), F32),
                pltpu.VMEM((count, heads, head), BF16),
                pltpu.VMEM((count, 1, LANES), F32),
                pltpu.VMEM((owned, n, heads, head), BF16),
                pltpu.VMEM((owned, n, 1, LANES), F32),
                dma((3, SLOTS)),
                dma((2, SENT + 1)),
                dma((2, owned)),
                dma((owned,)),
                dma((1,)),
                pltpu.VMEM((LAST, 2, half, head), F32),
                pltpu.VMEM((LAST, 2, half, head), BF16),
                pltpu.VMEM((LAST, half, head), BF16),
                pltpu.VMEM((LAST, 1, LANES), F32),
                pltpu.VMEM((LAST, half, head), BF16),
                pltpu.VMEM((LAST, 1, LANES), F32),
                pltpu.VMEM((LAST, n, half, head), BF16),
                pltpu.VMEM((LAST, n, 1, LANES), F32),
                dma((2, LAST)),
                dma((2, LAST)),
                dma((2, LAST)),
                dma((2, LAST)),
            ],
            compiler_params=pltpu.CompilerParams(collective_id=0, has_side_effects=True, vmem_limit_bytes=48 * 2**20),
        )(pltpu.with_memory_space_constraint(q, pltpu.HBM), k.reshape(-1, head), v.reshape(-1, head))

    return jax.shard_map(
        step,
        mesh=mesh,
        in_specs=(P("dp", None, None), P("dp", "sp", None, None), P("dp", "sp", None, None)),
        out_specs=P("dp", None, None),
        check_vma=False,
    )
```

```python
import functools

import jax
import jax.numpy as jnp
from jax import lax
from jax.experimental import pallas as pl
from jax.experimental.pallas import tpu as pltpu
from jax.sharding import PartitionSpec as P

F32, BF16 = jnp.float32, jnp.bfloat16
LOG2E = 1.4426950408889634
CHUNK = 32
SLOTS = 4
LAST = 3
DELAY = 3
SENT = 3
LANES = 128


def kernel(n, scale, q_hbm, k_hbm, v_hbm, out, q, keys, values, mask, scores, high, part, stats, parts, allstats, in_sem, to_sems, to_semr, res_sems, res_semr, mine, halves, pair, pairstats, both, bothstats, alls, allsstats, pair_sems, pair_semr, all_sems, all_semr, end_sems, end_semr, span):
    count, heads, head = out.shape
    rows = keys.shape[1]
    chunk = CHUNK * heads
    chunks = rows // chunk
    owned = pl.cdiv(count, n)
    early = count - LAST
    me = lax.axis_index("sp")

    def fetch(i, which):
        slot = lax.rem(i, SLOTS)
        cache, here = ((k_hbm, keys), (v_hbm, values))[which]
        return pltpu.make_async_copy(cache.at[pl.ds(i * rows, rows)], here.at[slot], in_sem.at[which, slot])

    q_copy = pltpu.make_async_copy(q_hbm, q, in_sem.at[2, 0])
    q_copy.start()
    fetch(0, 0).start()
    for i in range(1, SLOTS):
        fetch(i, 0).start()
        fetch(i - 1, 1).start()

    barrier = pltpu.get_barrier_semaphore()
    for step in range(1, n):
        pl.semaphore_signal(barrier, inc=1, device_id={"sp": lax.rem(me + step, n)})

    column = lax.broadcasted_iota(jnp.int32, (heads, chunk), 1).astype(F32)
    column = column - heads * jnp.floor((column + 0.5) * (1 / heads))
    row = lax.broadcasted_iota(jnp.int32, (heads, chunk), 0).astype(F32)
    mask[...] = jnp.where(column == row, jnp.inf, -jnp.inf)

    lane = lax.broadcasted_iota(jnp.int32, (heads, LANES), 1)
    line = lax.broadcasted_iota(jnp.int32, (heads, LANES), 0)
    own_lane = lane == line

    def score(i, place):
        slot = lax.rem(i, SLOTS)
        best = []

        def one(j):
            got = lax.dot_general(q[i], keys[slot, pl.ds(j * chunk, chunk), :], (((1,), (1,)), ((), ())), preferred_element_type=F32)
            got = jnp.minimum(got, mask[...])
            scores[place, :, pl.ds(j * chunk, chunk)] = got
            for g in range(chunk // LANES):
                piece = got[:, g * LANES : (g + 1) * LANES]
                best[:] = [jnp.maximum(best[0], piece) if best else piece]

        def end():
            high[place] = jnp.broadcast_to(jnp.max(best[0], -1, keepdims=True), (heads, LANES))

        return one, end

    def value(i, place):
        slot = lax.rem(i, SLOTS)
        top = high[place]
        total, seen = [], []

        def one(j):
            weights = []
            for g in range(chunk // LANES):
                w = jnp.exp2((scores[place, :, pl.ds(j * chunk + g * LANES, LANES)] - top) * (scale * LOG2E))
                total[:] = [total[0] + w if total else w]
                weights.append(w.astype(BF16))
            got = jnp.dot(jnp.concatenate(weights, 1), values[slot, pl.ds(j * chunk, chunk), :], preferred_element_type=F32)
            seen[:] = [seen[0] + got if seen else got]

        def end():
            sums = jnp.sum(total[0], -1, keepdims=True)
            known = jnp.where(own_lane, top, 0.0) + jnp.where(lane == line + LANES // 2, sums, 0.0)
            stats[i] = jnp.sum(known, 0, keepdims=True)
            return seen[0]

        return one, end

    def part_bytes(number, size, sem):
        ref = span.at[0 : number * (size * head // 2 // LANES + 1)]
        pltpu.make_async_copy(ref, ref, sem).wait()

    def owner(i):
        return lax.rem(i, n // 2) * 2 + lax.rem(i // (n // 2), 2)

    def to_owner(i):
        place, there, sem = i // n, owner(i), to_sems.at[lax.rem(i, SENT + 1)]
        return [
            pltpu.make_async_remote_copy(part.at[i], parts.at[place, me], sem, to_semr.at[place], device_id={"sp": there}),
            pltpu.make_async_remote_copy(stats.at[i], allstats.at[place, me], sem, to_semr.at[place], device_id={"sp": there}),
        ]

    def keep(i, place):
        parts[place, me] = part[i]
        allstats[place, me] = stats[i]

    def other(flips):
        there = me
        for bit in range(4):
            if flips >> bit & 1:
                there = there + (1 - 2 * lax.rem(me // 2**bit, 2)) * 2**bit
        return there

    order = sorted(range(1, n), key=lambda flips: (-bin(flips >> 1).count("1"), flips))
    chips = [flips for flips in order if flips % 2 == 0]

    core = lax.rem(me, 2)
    half = halves.shape[2]
    cuts = (0, heads - half)
    line_half = lax.broadcasted_iota(jnp.int32, (half, LANES), 0)
    lane_half = lax.broadcasted_iota(jnp.int32, (half, LANES), 1)
    low = lax.broadcasted_iota(jnp.int32, (1, LANES), 1) < LANES // 2

    def swap(which, i):
        there = other(1)
        return [
            pltpu.make_async_remote_copy(halves.at[which, 1 - core], pair.at[which], pair_sems.at[which], pair_semr.at[which], device_id={"sp": there}),
            pltpu.make_async_remote_copy(stats.at[i], pairstats.at[which], pair_sems.at[which], pair_semr.at[which], device_id={"sp": there}),
        ]

    def to_pair(i, seen):
        which = i - early
        for c, cut in enumerate(cuts):
            mine[which, c] = seen[cut : cut + half]
            halves[which, c] = seen[cut : cut + half].astype(BF16)
        for copy in swap(which, i):
            copy.start()

    def all_copies(which, there):
        return [
            pltpu.make_async_remote_copy(both.at[which], alls.at[which, me // 2], all_sems.at[which], all_semr.at[which], device_id={"sp": there}),
            pltpu.make_async_remote_copy(bothstats.at[which], allsstats.at[which, me // 2], all_sems.at[which], all_semr.at[which], device_id={"sp": there}),
        ]

    def to_all(i):
        which = i - early
        part_bytes(1, half, pair_semr.at[which])
        a, b = stats[i], pairstats[which]
        top = jnp.maximum(a, b)
        a_share, b_share = jnp.exp2((a - top) * (scale * LOG2E)), jnp.exp2((b - top) * (scale * LOG2E))
        sums = a_share * pltpu.roll(a, LANES // 2, 1) + b_share * pltpu.roll(b, LANES // 2, 1)
        known = jnp.where(low, top, pltpu.roll(sums, LANES // 2, 1))
        own = lane_half == line_half + core * cuts[1]
        a_share, b_share = (jnp.sum(jnp.where(own, jnp.broadcast_to(x, own.shape), 0.0), -1, keepdims=True) for x in (a_share, b_share))
        got = (a_share * mine[which, core] + b_share * pair[which].astype(F32)).astype(BF16)
        both[which] = got
        bothstats[which] = known
        for flips in chips:
            for copy in all_copies(which, other(flips)):
                copy.start()
        alls[which, me // 2] = got
        allsstats[which, me // 2] = known

    def end_copy(i, c):
        there = out.at[i, (0, half)[c] : (half, heads)[c]]
        return pltpu.make_async_remote_copy(there, there, end_sems.at[i - early], end_semr.at[i - early], device_id={"sp": other(1)})

    def combine_all(i):
        which = i - early
        part_bytes(n // 2 - 1, half, all_semr.at[which])
        share = shares(jnp.concatenate([allsstats[which, s] for s in range(n // 2)], 0))
        own = lane_half == line_half + core * cuts[1]
        got = None
        for s in range(n // 2):
            column = jnp.sum(jnp.where(own, jnp.broadcast_to(share[s : s + 1], own.shape), 0.0), -1, keepdims=True)
            term = column * alls[which, s].astype(F32)
            got = term if got is None else got + term

        @pl.when(core == 0)
        def _():
            out[i, :half] = got.astype(BF16)
            end_copy(i, 0).start()

        @pl.when(core == 1)
        def _():
            out[i, half:] = got[2 * half - heads :].astype(BF16)
            end_copy(i, 1).start()

    def shares(known):
        share = jnp.exp2((known - jnp.max(known, 0, keepdims=True)) * (scale * LOG2E))
        return share / jnp.sum(share * pltpu.roll(known, LANES // 2, 1), 0, keepdims=True)

    def combine(place, i):
        part_bytes(n - 1, heads, to_semr.at[place])
        share = shares(jnp.concatenate([allstats[place, s] for s in range(n)], 0))
        got = None
        for s in range(n):
            column = jnp.sum(jnp.where(own_lane, jnp.broadcast_to(share[s : s + 1], (heads, LANES)), 0.0), -1, keepdims=True)
            term = column * parts[place, s].astype(F32)
            got = term if got is None else got + term
        out[i] = got.astype(BF16)

    def finish(i):
        @pl.when(owner(i) == me)
        def _():
            place = i // n
            combine(place, i)
            for flips in order:
                pltpu.make_async_remote_copy(out.at[i], out.at[i], res_sems.at[place], res_semr.at[0], device_id={"sp": other(flips)}).start()

    def send(i):
        @pl.when(owner(i) != me)
        def _():
            for copy in to_owner(i):
                copy.start()

        @pl.when(owner(i) == me)
        def _():
            keep(i, i // n)

    def sent(i):
        @pl.when(owner(i) != me)
        def _():
            part_bytes(1, heads, to_sems.at[lax.rem(i, SENT + 1)])

    q_copy.wait()
    fetch(0, 0).wait()
    one, end = score(0, 0)
    for j in range(chunks):
        one(j)
    end()
    pl.semaphore_wait(barrier, n - 1)

    def step(i, _):
        fetch(i + SLOTS - 2, 1).start()

        @pl.when(i + SLOTS - 1 < count)
        def _():
            fetch(i + SLOTS - 1, 0).start()

        fetch(i, 0).wait()
        fetch(i - 1, 1).wait()
        value_one, value_end = value(i - 1, 0)
        score_one, score_end = score(i, 0)
        for j in range(chunks):
            value_one(j)
            score_one(j)
        last = i - 1
        part[last] = value_end().astype(BF16)
        score_end()

        send(last)

        @pl.when(last >= DELAY)
        def _():
            finish(last - DELAY)

        @pl.when(last >= SENT)
        def _():
            sent(last - SENT)

        return 0

    lax.fori_loop(1, count - 2, step, 0)

    def score_alone(i, place):
        fetch(i, 0).wait()
        one, end = score(i, place)
        for j in range(chunks):
            one(j)
        end()

    def value_alone(i, place):
        fetch(i, 1).wait()
        one, end = value(i, place)
        for j in range(chunks):
            one(j)
        return end()

    a, b, c = range(early, count)
    score_alone(b, 1)
    finish(early - 3)
    to_pair(a, value_alone(a, 0))
    score_alone(c, 0)
    to_all(a)
    finish(early - 2)
    to_pair(b, value_alone(b, 1))
    finish(early - 1)
    to_pair(c, value_alone(c, 0))
    to_all(b)
    to_all(c)
    for i in range(early, count):
        combine_all(i)

    for i in range(early - SENT, early):
        sent(i)
    most = pl.cdiv(early, n)
    for number in (most - 1, most):

        @pl.when((early + n - 1 - me // 2 - lax.rem(me, 2) * (n // 2)) // n == number)
        def _():
            ref = out.at[pl.ds(0, early - number)]
            pltpu.make_async_copy(ref, ref, res_semr.at[0]).wait()
            ref = out.at[pl.ds(0, n - 1)]
            for place in range(number):
                pltpu.make_async_copy(ref, ref, res_sems.at[place]).wait()

    for which in range(LAST):
        part_bytes(1, half, pair_sems.at[which])
        part_bytes(n // 2 - 1, half, all_sems.at[which])
    for c in (0, 1):

        @pl.when(core == c)
        def _():
            for i in range(early, count):
                end_copy(i, c).wait_send()
                end_copy(i, 1 - c).wait_recv()


def solution(mesh):
    n = mesh.shape["sp"]

    def step(q, k, v):
        count, tokens, heads, head = k.shape
        rows = tokens * heads
        owned = pl.cdiv(count, n)
        half = heads * 4 // 7
        anywhere = pl.BlockSpec(memory_space=pl.ANY)
        dma = pltpu.SemaphoreType.DMA
        return pl.pallas_call(
            functools.partial(kernel, n, head**-0.5),
            out_shape=jax.ShapeDtypeStruct(q.shape, BF16),
            in_specs=[pl.BlockSpec(memory_space=pltpu.HBM), anywhere, anywhere],
            out_specs=pl.BlockSpec(memory_space=pltpu.VMEM),
            scratch_shapes=[
                pltpu.VMEM(q.shape, BF16),
                pltpu.VMEM((SLOTS, rows, head), BF16),
                pltpu.VMEM((SLOTS, rows, head), BF16),
                pltpu.VMEM((heads, CHUNK * heads), F32),
                pltpu.VMEM((2, heads, rows), F32),
                pltpu.VMEM((2, heads, LANES), F32),
                pltpu.VMEM((count, heads, head), BF16),
                pltpu.VMEM((count, 1, LANES), F32),
                pltpu.VMEM((owned, n, heads, head), BF16),
                pltpu.VMEM((owned, n, 1, LANES), F32),
                dma((3, SLOTS)),
                dma((SENT + 1,)),
                dma((owned,)),
                dma((owned,)),
                dma((1,)),
                pltpu.VMEM((LAST, 2, half, head), F32),
                pltpu.VMEM((LAST, 2, half, head), BF16),
                pltpu.VMEM((LAST, half, head), BF16),
                pltpu.VMEM((LAST, 1, LANES), F32),
                pltpu.VMEM((LAST, half, head), BF16),
                pltpu.VMEM((LAST, 1, LANES), F32),
                pltpu.VMEM((LAST, n // 2, half, head), BF16),
                pltpu.VMEM((LAST, n // 2, 1, LANES), F32),
                dma((LAST,)),
                dma((LAST,)),
                dma((LAST,)),
                dma((LAST,)),
                dma((LAST,)),
                dma((LAST,)),
                pltpu.VMEM((n * (heads * head // 2 // LANES + 1), 1, LANES), F32),
            ],
            compiler_params=pltpu.CompilerParams(collective_id=0, has_side_effects=True, vmem_limit_bytes=48 * 2**20),
        )(pltpu.with_memory_space_constraint(q, pltpu.HBM), k.reshape(-1, head), v.reshape(-1, head))

    return jax.shard_map(
        step,
        mesh=mesh,
        in_specs=(P("dp", None, None), P("dp", "sp", None, None), P("dp", "sp", None, None)),
        out_specs=P("dp", None, None),
        check_vma=False,
    )
```
